32 devices in a mesh: grp: 4 (over x, core), shard: 8 (over z, y).
Axes of the slice: x: 2, y: 2, z: 4, core: 2. Of those that a mesh axis runs over, the one named last changes fastest.
Arguments:
- tokens: bfloat16 [1024, 1280], P('shard'), may hold values from -6 to 6
- fc1_mean: float32 [5120, 1280], P('shard'), may hold values from -0.15625 to 0.15625
- fc1_variance: float32 [5120, 1280], P('shard'), may hold values from 1e-05 to 0.001
- fc1_deviation: bfloat16 [20, 5120, 1280], P(None, 'shard'), may hold values from -0.19921875 to 0.19921875
- fc2_mean: float32 [1280, 5120], P(None, 'shard'), may hold values from -0.078125 to 0.078125
- fc2_variance: float32 [1280, 5120], P(None, 'shard'), may hold values from 2.5e-06 to 0.00025
- fc2_deviation: bfloat16 [20, 1280, 5120], P(None, None, 'shard'), may hold values from -0.099609375 to 0.099609375
- noise_fc1: bfloat16 [8, 5120, 1280], P('grp', 'shard'), may hold values from -6 to 6
- noise_fc2: bfloat16 [8, 1280, 5120], P('grp', None, 'shard'), may hold values from -6 to 6
- noise_low: float32 [8, 20], P('grp'), may hold values from -4 to 4
Outputs:
- prediction: bfloat16 [1024, 1280], P('shard', 'grp')
The draws below stay inside these ranges and needn't reach their ends.
All inputs are finite; a program needn't handle non-finite values.
Results may differ from the reference program's by a relative error of at most 0.013.
Values may be sent and summed in bfloat16 or wider, within the bound.
A program may use at most 256 MiB of HBM per device.

```python
import math
import jax
import jax.numpy as jnp
from jax import lax

D = 1280
FF = 5120
K = 20
SAMPLES = 8
TOKENS = 1024


def block_levels(own_key, dims, cuts, least, largest):
    gain, own = 1.0, jax.random.fold_in(own_key, 6)
    for axis_at, parts in cuts:
        steps = jnp.exp(jax.random.uniform(jax.random.fold_in(own, axis_at), (parts,), jnp.float32, least / len(cuts), largest / len(cuts)))
        gain = gain * jnp.repeat(steps, dims[axis_at] // parts).reshape([-1 if axis == axis_at else 1 for axis in range(len(dims))])
    return gain


def bell_draw(own_key, dims, scale, most, split=(), kind=jnp.bfloat16):
    values = scale * jax.random.normal(own_key, dims, jnp.float32)
    if split:
        values = values * block_levels(own_key, dims, split, -0.22, 0.18)
    return jnp.clip(values, -most, most).astype(kind)


def setup_inputs(seed: int = 0) -> dict:
    arg_keys = jax.random.split(jax.random.key(seed), 11)
    return {
        "tokens": bell_draw(arg_keys[0], (TOKENS, D), 1.0, 6.0, ((0, 8),)),
        "fc1_mean": bell_draw(arg_keys[1], (FF, D), D ** -0.5, 0.15625, ((0, 8),), jnp.float32),
        "fc1_variance": jnp.clip(jnp.exp(math.log(0.001) - 4.6051703 * jax.random.uniform(arg_keys[2], (FF, D), jnp.float32) ** block_levels(arg_keys[2], (FF, D), ((0, 8),), -0.2, 0.2)), 9.999999747378752e-06, 0.001),
        "fc1_deviation": bell_draw(arg_keys[3], (K, FF, D), 0.03, 0.19921875, ((1, 8),)),
        "fc2_mean": bell_draw(arg_keys[4], (D, FF), FF ** -0.5, 0.078125, ((1, 8),), jnp.float32),
        "fc2_variance": jnp.clip(jnp.exp(math.log(0.00025) - 4.6051703 * jax.random.uniform(arg_keys[5], (D, FF), jnp.float32) ** block_levels(arg_keys[5], (D, FF), ((1, 8),), -0.2, 0.2)), 2.499999936844688e-06, 0.00025),
        "fc2_deviation": bell_draw(arg_keys[6], (K, D, FF), 0.015, 0.099609375, ((2, 8),)),
        "noise_fc1": bell_draw(arg_keys[7], (SAMPLES, FF, D), 1.0, 6.0, ((0, 4), (1, 8))),
        "noise_fc2": bell_draw(arg_keys[8], (SAMPLES, D, FF), 1.0, 6.0, ((0, 4), (2, 8))),
        "noise_low": bell_draw(arg_keys[9], (SAMPLES, K), 1.0, 4.0, ((0, 4),), jnp.float32),
    }


def sample_weights(moment_mean, moment_variance, deviation, noise_diag, low_half):
    columns = deviation.shape[0]
    flattened = deviation.reshape(columns, -1)
    low_rank = jnp.dot(low_half, flattened, preferred_element_type=jnp.float32)
    low_rank = low_rank.reshape((low_half.shape[0],) + moment_mean.shape)
    sampled = moment_mean[None] + jnp.sqrt(moment_variance)[None] * noise_diag.astype(jnp.float32)
    sampled = sampled + low_rank / math.sqrt(2.0 * (columns - 1))
    return sampled.astype(jnp.bfloat16)

def reference(tokens, fc1_mean, fc1_variance, fc1_deviation, fc2_mean, fc2_variance, fc2_deviation, noise_fc1, noise_fc2, noise_low):
    low_half = noise_low.astype(jnp.bfloat16)
    up_weights = sample_weights(fc1_mean, fc1_variance, fc1_deviation, noise_fc1, low_half)
    down_weights = sample_weights(fc2_mean, fc2_variance, fc2_deviation, noise_fc2, low_half)

    def accumulate(running, weight_pair):
        first_w, second_w = weight_pair
        preact = jnp.dot(tokens, first_w.T, preferred_element_type=jnp.float32)
        hidden = jax.nn.gelu(preact, approximate=False).astype(jnp.bfloat16)
        return (running + jnp.dot(hidden, second_w.T, preferred_element_type=jnp.float32), None)
    start_sum = jnp.zeros((tokens.shape[0], tokens.shape[1]), jnp.float32)
    summed, _ = lax.scan(accumulate, start_sum, (up_weights, down_weights))
    return (summed / SAMPLES).astype(jnp.bfloat16)
```

```python
import functools
import math

import jax
import jax.numpy as jnp
from jax import lax
from jax.experimental import pallas as pl
from jax.experimental.pallas import tpu as pltpu
from jax.sharding import PartitionSpec as P

UNIT = 32


def from_partner(value, axis, mask):
    pairs = [(source, source ^ mask) for source in range(lax.axis_size(axis))]
    return lax.ppermute(value, axis, pairs)


def sample_kernel(scale, unit, order_ref, spread_ref, mean_ref, variance_ref, deviation_ref, noise_ref, out_ref):
    samples = noise_ref.shape[0]
    columns, rows, width = deviation_ref.shape

    def step(i, carry):
        at = pl.ds(pl.multiple_of(i * unit, unit), unit)
        stacked = deviation_ref[:, at, :].reshape(columns * unit, width)
        low_rank = jnp.dot(spread_ref[...], stacked, preferred_element_type=jnp.float32)
        mean = mean_ref[at, :]
        std = jnp.sqrt(variance_ref[at, :])
        for s in range(samples):
            part = low_rank[s * unit : (s + 1) * unit]
            value = mean + std * noise_ref[s, at, :].astype(jnp.float32) + part * scale
            out_ref[s, at, :] = value.astype(out_ref.dtype)
        return carry

    lax.fori_loop(0, rows // unit, step, 0)


def sample_weights(order, parts, mean, variance, deviation, noise, low_half, name):
    columns, rows, width = deviation.shape
    samples = noise.shape[0]
    per_part = rows // parts
    unit = math.gcd(UNIT, per_part)
    block = max(
        b
        for b in range(unit, per_part + 1, unit)
        if per_part % b == 0 and (b == unit or columns * b * width * 2 <= 4500000)
    )
    steps = per_part // block
    eye = jnp.eye(unit, dtype=jnp.bfloat16)
    spread = (low_half[:, None, :, None] * eye[None, :, None, :]).reshape(samples * unit, columns * unit)

    def source(i, order):
        return order[i // steps] * steps + i % steps

    count = rows * width
    return pl.pallas_call(
        functools.partial(sample_kernel, 1.0 / math.sqrt(2.0 * (columns - 1)), unit),
        grid_spec=pltpu.PrefetchScalarGridSpec(
            num_scalar_prefetch=1,
            grid=(parts * steps,),
            in_specs=[
                pl.BlockSpec(spread.shape, lambda i, o: (0, 0)),
                pl.BlockSpec((block, width), lambda i, o: (source(i, o), 0)),
                pl.BlockSpec((block, width), lambda i, o: (source(i, o), 0)),
                pl.BlockSpec((columns, block, width), lambda i, o: (0, source(i, o), 0)),
                pl.BlockSpec((samples, block, width), lambda i, o: (0, source(i, o), 0)),
            ],
            out_specs=pl.BlockSpec((samples, block, width), lambda i, o: (0, i, 0)),
        ),
        out_shape=jax.ShapeDtypeStruct((samples, rows, width), jnp.bfloat16),
        cost_estimate=pl.CostEstimate(
            flops=2 * count * columns * samples,
            bytes_accessed=count * (2 * columns + 8 + 4 * samples),
            transcendentals=count,
        ),
        compiler_params=pltpu.CompilerParams(
            dimension_semantics=("arbitrary",), vmem_limit_bytes=60 * 1024 * 1024
        ),
        name=name,
    )(order, spread, mean, variance, deviation, noise)


def mlp_kernel(rows, core_ref, own_ref, other_ref, up_ref, down_ref, *out_refs):
    half = own_ref.shape[1]
    pairs, kept, piece = out_refs[0].shape
    core = core_ref[0]
    own_at = pl.ds(pl.multiple_of(core * half, half), half)
    other_at = pl.ds(pl.multiple_of((1 - core) * half, half), half)
    across = (((1,), (1,)), ((), ()))
    total = None
    for s in range(up_ref.shape[0]):
        preact = lax.dot_general(own_ref[...], up_ref[s, :, own_at], across, preferred_element_type=jnp.float32)
        preact += lax.dot_general(other_ref[...], up_ref[s, :, other_at], across, preferred_element_type=jnp.float32)
        hidden = (0.5 * preact * (1.0 + lax.erf(preact * math.sqrt(0.5)))).astype(jnp.bfloat16)
        term = lax.dot_general(hidden, down_ref[s], across, preferred_element_type=jnp.float32)
        total = term if total is None else total + term
    for p in range(2 * pairs):
        part = total[:, p * piece : (p + 1) * piece].astype(out_refs[0].dtype)
        part = part.reshape(2 * kept // rows, 2, rows // 2, piece)
        for stream in range(2):
            out_refs[2 * (p % 2) + stream][p // 2] = part[:, stream].reshape(kept, piece)


def mlp(core, own, other, up, down, parts, rows):
    tokens, half = own.shape
    samples, hidden, width = up.shape
    block = min(tokens, rows * max(1, 256 // rows))
    piece = width // parts
    return pl.pallas_call(
        functools.partial(mlp_kernel, rows),
        grid_spec=pltpu.PrefetchScalarGridSpec(
            num_scalar_prefetch=1,
            grid=(tokens // block,),
            in_specs=[
                pl.BlockSpec((block, half), lambda i, c: (i, 0)),
                pl.BlockSpec((block, half), lambda i, c: (i, 0)),
                pl.BlockSpec(up.shape, lambda i, c: (0, 0, 0)),
                pl.BlockSpec(down.shape, lambda i, c: (0, 0, 0)),
            ],
            out_specs=[pl.BlockSpec((parts // 2, block // 2, piece), lambda i, c: (0, i, 0))] * 4,
        ),
        out_shape=[jax.ShapeDtypeStruct((parts // 2, tokens // 2, piece), jnp.bfloat16)] * 4,
        cost_estimate=pl.CostEstimate(
            flops=4 * tokens * samples * hidden * width,
            bytes_accessed=2 * (2 * tokens * width + 2 * samples * hidden * width),
            transcendentals=tokens * samples * hidden,
        ),
        compiler_params=pltpu.CompilerParams(
            dimension_semantics=("arbitrary",), vmem_limit_bytes=60 * 1024 * 1024
        ),
        name="mlp",
    )(core, own, other, up, down)


def fold(value, axis, mask, dim):
    kept = lax.index_in_dim(value, 0, dim, keepdims=True)
    sent = lax.index_in_dim(value, 1, dim, keepdims=True).astype(jnp.bfloat16)
    return kept.astype(jnp.float32) + from_partner(sent, axis, mask).astype(jnp.float32)


MESH_ID = pl.DeviceIdType.MESH
SLOTS = 8


def fused_kernel(
    cfg,
    low_ref,
    tokens_ref,
    mean1_ref,
    var1_ref,
    dev1_ref,
    mean2_ref,
    var2_ref,
    dev2_ref,
    noise1_ref,
    noise2_ref,
    out_ref,
    lowbuf,
    spread4,
    spread2,
    tok,
    dbuf1,
    mbuf1,
    nz1,
    up,
    dbuf2,
    mbuf2,
    nz2,
    down,
    hid,
    s1send,
    s1keep,
    s1recv,
    s2send,
    s2keep,
    s2recv,
    s3send,
    s3recv,
    fin,
    sem_ld1,
    sem_ld2,
    sem_tok,
    sem_low,
    sem_n1,
    sem_n2,
    sem_z,
    sem_y,
    sem_d,
    sem_h,
    sem_x1,
    sem_y2,
    sem_z3,
):
    unit, main, mid, rows2, scale, total_samples = cfg
    columns = dev1_ref.shape[0]
    hidden = dev1_ref.shape[1]
    width = dev1_ref.shape[2]
    own_samples = noise1_ref.shape[0]
    samples = 2 * own_samples
    block, _ = tokens_ref.shape
    half = width // 2
    piece = out_ref.shape[1]
    n_mid, n_main = mid // unit, main // unit
    n1 = n_mid + n_main
    n2 = 2 * piece // rows2
    steps = lax.axis_size("shard") // 2

    g = lax.axis_index("grp")
    s = lax.axis_index("shard")
    c = g % 2
    x = g // 2
    y = s % 2
    z = s // 2
    partner = (g ^ 1, s)
    xn = (g ^ 2, s)
    yn = (g, s ^ 1)
    middle = jnp.logical_or(z == 1, z == 2)

    def zn(k):
        return (g, s ^ (2 * k))

    def remote(src, dst, sems, index, device):
        return pltpu.make_async_remote_copy(
            src_ref=src,
            dst_ref=dst,
            send_sem=sems.at[(0,) + index],
            recv_sem=sems.at[(1,) + index],
            device_id=device,
            device_id_type=MESH_ID,
        )

    def copies1(i):
        slot = i % SLOTS
        at_mid = i < n_mid
        row = pl.multiple_of(jnp.where(at_mid, main + i * unit, c * (main + mid) + (i - n_mid) * unit), unit)
        place = pl.multiple_of(jnp.where(at_mid, main + i * unit, (i - n_mid) * unit), unit)
        src = pl.ds(row, unit)
        own = pl.ds(own_samples * c, own_samples)
        return (
            pltpu.make_async_copy(dev1_ref.at[:, src, :], dbuf1.at[slot], sem_ld1.at[slot, 0]),
            pltpu.make_async_copy(mean1_ref.at[src, :], mbuf1.at[slot, 0], sem_ld1.at[slot, 1]),
            pltpu.make_async_copy(var1_ref.at[src, :], mbuf1.at[slot, 1], sem_ld1.at[slot, 2]),
            pltpu.make_async_copy(noise1_ref.at[:, src, :], nz1.at[own, pl.ds(place, unit), :], sem_ld1.at[slot, 3]),
        )

    def feature_row(core, j):
        per = n2 // 2
        first = j < per
        chip = jnp.where(first, 1 - x, x)
        inner = jnp.where(first, j, j - per)
        return pl.multiple_of(chip * 2 * piece + core * piece + inner * rows2, math.gcd(piece, rows2))

    def copies2(j):
        slot = j % SLOTS
        src = pl.ds(feature_row(c, j), rows2)
        own = pl.ds(own_samples * c, own_samples)
        to = pl.ds(pl.multiple_of(j * rows2, rows2), rows2)
        return (
            pltpu.make_async_copy(dev2_ref.at[:, src, :], dbuf2.at[slot], sem_ld2.at[slot, 0]),
            pltpu.make_async_copy(mean2_ref.at[src, :], mbuf2.at[slot, 0], sem_ld2.at[slot, 1]),
            pltpu.make_async_copy(var2_ref.at[src, :], mbuf2.at[slot, 1], sem_ld2.at[slot, 2]),
            pltpu.make_async_copy(noise2_ref.at[:, src, :], nz2.at[own, to, :], sem_ld2.at[slot, 3]),
        )

    def start(copies):
        for copy in copies:
            copy.start()

    def wait(copies):
        for copy in copies:
            copy.wait()

    own_tokens = pltpu.make_async_copy(tokens_ref, tok.at[s], sem_tok)
    own_tokens.start()
    for i in range(min(SLOTS, n1)):
        start(copies1(jnp.int32(i)))

    barrier = pltpu.get_barrier_semaphore()
    peers = [partner, xn, yn] + [zn(k) for k in range(1, steps)]
    for peer in peers:
        pl.semaphore_signal(barrier, inc=1, device_id=peer, device_id_type=MESH_ID)

    def start_later(q):
        @pl.when(q < n1)
        def _():
            start(copies1(q))

        @pl.when(jnp.logical_and(q >= n1, q < n1 + n2))
        def _():
            start(copies2(q - n1))

    def spread_of(low):
        count = low.shape[0]
        pick = lax.broadcasted_iota(jnp.int32, (columns, columns * unit), 1) // unit
        pick = (pick == lax.broadcasted_iota(jnp.int32, (columns, columns * unit), 0)).astype(jnp.bfloat16)
        wide = jnp.dot(low.astype(jnp.bfloat16), pick, preferred_element_type=jnp.float32)
        lane = lax.broadcasted_iota(jnp.int32, (unit, columns * unit), 1) % unit
        eye = lane == lax.broadcasted_iota(jnp.int32, (unit, columns * unit), 0)
        parts = [jnp.where(eye, wide[i : i + 1, :], 0.0) for i in range(count)]
        return [p.astype(jnp.bfloat16) for p in parts]

    mine = spread_of(low_ref[...])
    for i in range(own_samples):
        spread2[pl.ds(i * unit, unit), :] = mine[i]

    def mid_step(i, carry):
        slot = i % SLOTS
        wait(copies1(i))
        stacked = dbuf1[slot].reshape(columns * unit, width)
        low_rank = jnp.dot(spread2[...], stacked, preferred_element_type=jnp.float32)
        mean = mbuf1[slot, 0]
        std = jnp.sqrt(mbuf1[slot, 1])
        from_row = pl.ds(pl.multiple_of(main + i * unit, unit), unit)
        for n in range(own_samples):
            noise = nz1[own_samples * c + n, from_row, :].astype(jnp.float32)
            value = mean + std * noise + low_rank[n * unit : (n + 1) * unit] * scale
            to = pl.ds(pl.multiple_of(samples * main + n * mid + i * unit, unit), unit)
            up[to, :] = value.astype(up.dtype)
        start_later(i + SLOTS)
        return carry

    lax.fori_loop(0, n_mid, mid_step, 0)

    own_tokens.wait()
    pl.semaphore_wait(barrier, len(peers))

    lanes = pl.ds(pl.multiple_of(c * half, half), half)

    def low_copy():
        return remote(low_ref, lowbuf, sem_low, (), partner)

    def noise1_copy(i):
        src = pl.ds(pl.multiple_of((1 - c) * (main + mid) + i * unit, unit), unit)
        to = pl.ds(pl.multiple_of(i * unit, unit), unit)
        own = pl.ds(own_samples * c, own_samples)
        return remote(noise1_ref.at[:, src, :], nz1.at[own, to, :], sem_n1, (i,), partner)

    def noise1_arrival(i):
        src = pl.ds(pl.multiple_of((1 - c) * (main + mid) + i * unit, unit), unit)
        to = pl.ds(pl.multiple_of(i * unit, unit), unit)
        other = pl.ds(own_samples * (1 - c), own_samples)
        return remote(noise1_ref.at[:, src, :], nz1.at[other, to, :], sem_n1, (i,), partner)

    def noise2_copy(j):
        src = pl.ds(feature_row(1 - c, j), rows2)
        to = pl.ds(pl.multiple_of(j * rows2, rows2), rows2)
        own = pl.ds(own_samples * c, own_samples)
        return remote(noise2_ref.at[:, src, :], nz2.at[own, to, :], sem_n2, (j,), partner)

    def noise2_arrival(j):
        src = pl.ds(feature_row(1 - c, j), rows2)
        to = pl.ds(pl.multiple_of(j * rows2, rows2), rows2)
        other = pl.ds(own_samples * (1 - c), own_samples)
        return remote(noise2_ref.at[:, src, :], nz2.at[other, to, :], sem_n2, (j,), partner)

    def token_copy(shard, sems, index, device):
        ref = tok.at[shard, :, lanes]
        return remote(ref, ref, sems, index, device)

    def z_copy(k):
        return token_copy(s, sem_z, (k,), zn(k))

    def z_arrival(k):
        return token_copy(s ^ (2 * k), sem_z, (k,), zn(k))

    def forward_copy():
        return token_copy(s ^ 4, sem_z, (3,), zn(1))

    def y_copy(k):
        return token_copy(s ^ (2 * k), sem_y, (k,), yn)

    def y_arrival(k):
        return token_copy(s ^ (2 * k) ^ 1, sem_y, (k,), yn)

    def d_copy(k, side):
        return token_copy(s ^ (2 * k) ^ side, sem_d, (k, side), partner)

    def d_arrival(k, side):
        other = pl.ds(pl.multiple_of((1 - c) * half, half), half)
        ref = tok.at[s ^ (2 * k) ^ side, :, other]
        return remote(ref, ref, sem_d, (k, side), partner)

    low_copy().start()
    for i in range(n_main):
        noise1_copy(i).start()
    z_copy(1).start()
    y_copy(0).start()
    z_copy(2).start()

    @pl.when(middle)
    def _():
        z_copy(3).start()

    for j in range(n2):
        noise2_copy(j).start()

    low_copy().wait_recv()
    others = spread_of(lowbuf[...])
    for i in range(own_samples):
        first = c == 0
        spread4[pl.ds(i * unit, unit), :] = jnp.where(first, mine[i], others[i])
        spread4[pl.ds((own_samples + i) * unit, unit), :] = jnp.where(first, others[i], mine[i])

    def main_step(i, carry):
        q = i + n_mid
        slot = q % SLOTS
        wait(copies1(q))
        noise1_arrival(i).wait_recv()
        stacked = dbuf1[slot].reshape(columns * unit, width)
        low_rank = jnp.dot(spread4[...], stacked, preferred_element_type=jnp.float32)
        mean = mbuf1[slot, 0]
        std = jnp.sqrt(mbuf1[slot, 1])
        from_row = pl.ds(pl.multiple_of(i * unit, unit), unit)
        for n in range(samples):
            noise = nz1[n, from_row, :].astype(jnp.float32)
            value = mean + std * noise + low_rank[n * unit : (n + 1) * unit] * scale
            up[pl.ds(pl.multiple_of(n * main + i * unit, unit), unit), :] = value.astype(up.dtype)
        start_later(q + SLOTS)
        return carry

    def down_step(j, carry):
        slot = j % SLOTS
        wait(copies2(j))
        noise2_arrival(j).wait_recv()
        per_core = samples * main + own_samples * mid
        for u in range(rows2 // unit):
            inner = pl.ds(u * unit, unit)
            at = pl.ds(pl.multiple_of(j * rows2 + u * unit, unit), unit)
            stacked = dbuf2[slot, :, inner, :].reshape(columns * unit, hidden)
            low_rank = jnp.dot(spread4[...], stacked, preferred_element_type=jnp.float32)
            mean = mbuf2[slot, 0, inner, :]
            std = jnp.sqrt(mbuf2[slot, 1, inner, :])
            for n in range(samples):
                noise = nz2[n, at, :].astype(jnp.float32)
                value = mean + std * noise + low_rank[n * unit : (n + 1) * unit] * scale
                value = value.astype(down.dtype)
                holder, local = n // own_samples, n % own_samples
                down[at, pl.ds(n * main, main)] = value[:, :main]
                down[at, pl.ds(per_core + n * main, main)] = value[:, main + mid :]
                down[at, pl.ds(holder * per_core + samples * main + local * mid, mid)] = value[:, main : main + mid]
        start_later(n1 + j + SLOTS)
        return carry

    def hidden_copy(k):
        ref = hid.at[c, k]
        return remote(ref, ref, sem_h, (k,), partner)

    def hidden_arrival(k):
        ref = hid.at[1 - c, k]
        return remote(ref, ref, sem_h, (k,), partner)

    across = (((1,), (1,)), ((), ()))
    tile = 2 * mid

    def pre(k):
        zz = z ^ k
        if k:
            d_arrival(k, 0).wait_recv()
        d_arrival(k, 1).wait_recv()
        held = tok[pl.ds(2 * zz, 2), :, :].reshape(2 * block, width)

        def part(n, carry):
            at = pl.ds(pl.multiple_of(n * tile, tile), tile)
            preact = lax.dot_general(held, up[at, :], across, preferred_element_type=jnp.float32)
            value = 0.5 * preact * (1.0 + lax.erf(preact * math.sqrt(0.5)))
            hid[c, k, :, at] = value.astype(hid.dtype)
            return carry

        lax.fori_loop(0, hid.shape[3] // tile, part, 0)
        hidden_copy(k).start()

    def x_copy(k):
        return remote(s1send.at[k], s1recv.at[k], sem_x1, (k,), xn)

    def y2_copy(k):
        return remote(s2send.at[k], s2recv.at[k], sem_y2, (k,), yn)

    def z3_copy(k):
        return remote(s3send.at[k], s3recv.at[k], sem_z3, (k,), zn(k))

    def post(k):
        hidden_arrival(k).wait_recv()
        per_core = hid.shape[3]
        total = lax.dot_general(hid[0, k], down[:, :per_core], across, preferred_element_type=jnp.float32)
        total += lax.dot_general(hid[1, k], down[:, per_core:], across, preferred_element_type=jnp.float32)
        s1send[k] = total[:, :piece].astype(s1send.dtype).reshape(2, block, piece)
        x_copy(k).start()
        s1keep[k] = total[:, piece:].reshape(2, block, piece)

    def stage2(k):
        x_copy(k).wait_recv()
        sent = s1keep[k, 1 - y] + s1recv[k, 1 - y].astype(jnp.float32)
        s2send[k] = sent.astype(s2send.dtype)
        y2_copy(k).start()
        s2keep[k] = s1keep[k, y] + s1recv[k, y].astype(jnp.float32)

    def stage3(k):
        y2_copy(k).wait_recv()
        value = s2keep[k] + s2recv[k].astype(jnp.float32)
        if k == 0:
            fin[...] = value
        else:
            s3send[k] = value.astype(s3send.dtype)
            z3_copy(k).start()

    def z_hook(k):
        z_arrival(k).wait_recv()
        if k == 2:
            @pl.when(middle)
            def _():
                forward_copy().start()
        y_copy(k).start()
        d_copy(k, 0).start()

    def y_hook(k):
        y_arrival(k).wait_recv()
        d_copy(k, 1).start()

    lax.fori_loop(0, n_main, main_step, 0)
    y_hook(0)
    z_hook(1)
    lax.fori_loop(0, n2 // 2, down_step, 0)
    z_hook(2)
    y_hook(1)
    pre(0)
    lax.fori_loop(n2 // 2, n2, down_step, 0)
    z_hook(3)
    y_hook(2)
    pre(1)
    post(0)
    y_hook(3)
    pre(2)
    post(1)
    stage2(0)
    pre(3)
    post(2)
    stage2(1)
    stage3(0)
    post(3)
    stage2(2)
    stage3(1)
    stage2(3)
    stage3(2)
    stage3(3)
    result = fin[...]
    for k in range(1, steps):
        z3_copy(k).wait_recv()
        result = result + s3recv[k].astype(jnp.float32)
    out_ref[...] = (result / total_samples).astype(out_ref.dtype)

    low_copy().wait_send()
    for i in range(n_main):
        noise1_copy(i).wait_send()
    for j in range(n2):
        noise2_copy(j).wait_send()
    z_copy(1).wait_send()
    z_copy(2).wait_send()

    @pl.when(middle)
    def _():
        z_copy(3).wait_send()
        forward_copy().wait_send()

    for k in range(steps):
        y_copy(k).wait_send()
        d_copy(k, 1).wait_send()
        hidden_copy(k).wait_send()
        x_copy(k).wait_send()
        y2_copy(k).wait_send()
        if k:
            d_copy(k, 0).wait_send()
            z3_copy(k).wait_send()


def fused(
    tokens,
    fc1_mean,
    fc1_variance,
    fc1_deviation,
    fc2_mean,
    fc2_variance,
    fc2_deviation,
    noise_fc1,
    noise_fc2,
    noise_low,
):
    columns, hidden, width = fc1_deviation.shape
    own = noise_fc1.shape[0]
    samples = 2 * own
    groups = lax.axis_size("grp")
    shards = lax.axis_size("shard")
    steps = shards // 2
    block = tokens.shape[0]
    piece = width // groups
    tiles = hidden // 128
    main = tiles // 2 * 128
    mid = hidden - 2 * main
    unit = UNIT
    rows2 = 2 * unit
    n_main = main // unit
    n2 = 2 * piece // rows2
    per_core = samples * main + own * mid
    cfg = (unit, main, mid, rows2, 1.0 / math.sqrt(2.0 * (columns - 1)), own * groups)
    hbm = pl.BlockSpec(memory_space=pltpu.HBM)
    vmem = pl.BlockSpec(memory_space=pltpu.VMEM)
    bf16, f32 = jnp.bfloat16, jnp.float32
    dma = pltpu.SemaphoreType.DMA
    return pl.pallas_call(
        functools.partial(fused_kernel, cfg),
        out_shape=jax.ShapeDtypeStruct((block, piece), bf16),
        in_specs=[vmem] + [hbm] * 9,
        out_specs=vmem,
        scratch_shapes=[
            pltpu.VMEM(noise_low.shape, f32),
            pltpu.VMEM((samples * unit, columns * unit), bf16),
            pltpu.VMEM((own * unit, columns * unit), bf16),
            pltpu.VMEM((shards, block, width), bf16),
            pltpu.VMEM((SLOTS, columns, unit, width), bf16),
            pltpu.VMEM((SLOTS, 2, unit, width), f32),
            pltpu.VMEM((samples, main + mid, width), bf16),
            pltpu.VMEM((per_core, width), bf16),
            pltpu.VMEM((SLOTS, columns, rows2, hidden), bf16),
            pltpu.VMEM((SLOTS, 2, rows2, hidden), f32),
            pltpu.VMEM((samples, 2 * piece, hidden), bf16),
            pltpu.VMEM((2 * piece, 2 * per_core), bf16),
            pltpu.VMEM((2, steps, 2 * block, per_core), bf16),
            pltpu.VMEM((steps, 2, block, piece), bf16),
            pltpu.VMEM((steps, 2, block, piece), f32),
            pltpu.VMEM((steps, 2, block, piece), bf16),
            pltpu.VMEM((steps, block, piece), bf16),
            pltpu.VMEM((steps, block, piece), f32),
            pltpu.VMEM((steps, block, piece), bf16),
            pltpu.VMEM((steps, block, piece), bf16),
            pltpu.VMEM((steps, block, piece), bf16),
            pltpu.VMEM((block, piece), f32),
            dma((SLOTS, 4)),
            dma((SLOTS, 4)),
            dma,
            dma((2,)),
            dma((2, n_main)),
            dma((2, n2)),
            dma((2, steps)),
            dma((2, steps)),
            dma((2, steps, 2)),
            dma((2, steps)),
            dma((2, steps)),
            dma((2, steps)),
            dma((2, steps)),
        ],
        compiler_params=pltpu.CompilerParams(
            collective_id=0, has_side_effects=True, vmem_limit_bytes=67043328
        ),
        name="swag",
    )(
        noise_low,
        tokens,
        fc1_mean,
        fc1_variance,
        fc1_deviation,
        fc2_mean,
        fc2_variance,
        fc2_deviation,
        noise_fc1,
        noise_fc2,
    )


def fits_fused(groups, shards, tokens, deviation):
    width, hidden = tokens.shape[1], deviation.shape[1]
    return (
        groups == 4
        and shards == 8
        and hidden % 128 == 0
        and hidden // 128 % 2 == 1
        and width % 256 == 0
        and width // groups % (2 * UNIT) == 0
        and tokens.shape[0] % 16 == 0
    )


def body(
    tokens,
    fc1_mean,
    fc1_variance,
    fc1_deviation,
    fc2_mean,
    fc2_variance,
    fc2_deviation,
    noise_fc1,
    noise_fc2,
    noise_low,
):
    groups = lax.axis_size("grp")
    shard_count = lax.axis_size("shard")
    if fits_fused(groups, shard_count, tokens, fc1_deviation):
        return fused(
            tokens,
            fc1_mean,
            fc1_variance,
            fc1_deviation,
            fc2_mean,
            fc2_variance,
            fc2_deviation,
            noise_fc1,
            noise_fc2,
            noise_low,
        )
    low_half = noise_low.astype(jnp.bfloat16)
    samples = noise_fc1.shape[0] * groups
    hid_ways = min(8, shard_count)
    low_bits = (shard_count // hid_ways).bit_length() - 1
    tok_bits = hid_ways.bit_length() - 1
    grp_bits = groups.bit_length() - 1
    position = lax.axis_index("shard")
    group = lax.axis_index("grp")
    core = group % 2
    rows, width = tokens.shape
    half = width // 2

    mine = lax.dynamic_slice_in_dim(tokens, core * half, half, 1)
    gathered = [mine] + [from_partner(mine, "shard", m << low_bits) for m in range(1, hid_ways)]

    order = jnp.bitwise_xor(jnp.arange(groups, dtype=jnp.int32), group.astype(jnp.int32))
    whole = jnp.zeros((1,), jnp.int32)
    up = sample_weights(whole, 1, fc1_mean, fc1_variance, fc1_deviation, noise_fc1, low_half, "sample_up")
    down = sample_weights(order, groups, fc2_mean, fc2_variance, fc2_deviation, noise_fc2, low_half, "sample_down")
    for bit in range(low_bits):
        upper = position >> bit & 1 == 1
        partner = from_partner(up, "shard", 1 << bit)
        up = jnp.where(upper, jnp.concatenate([partner, up], 1), jnp.concatenate([up, partner], 1))
        partner = from_partner(down, "shard", 1 << bit)
        down = jnp.where(upper, jnp.concatenate([partner, down], 2), jnp.concatenate([down, partner], 2))

    gathered, up, down = lax.optimization_barrier((gathered, up, down))
    own = jnp.concatenate(gathered, 0)
    other = from_partner(own, "grp", 1)
    piece = width // groups
    kept_and_sent = mlp(core.astype(jnp.int32).reshape(1), own, other, up, down, groups, rows)
    grp_steps = [("grp", 1 << b, grp_bits - 1 - b) for b in range(1, grp_bits)]
    shard_steps = [("shard", 1 << (low_bits + b), grp_bits + tok_bits - 2 - b) for b in range(tok_bits)]
    first, second, rest = grp_steps, shard_steps[:1], shard_steps[:0:-1]
    done = []
    for stream, steps in enumerate((first + second + rest, second + first + rest)):
        swapped = from_partner(kept_and_sent[2 + stream], "grp", 1)
        part = kept_and_sent[stream].astype(jnp.float32) + swapped.astype(jnp.float32)
        part = part.reshape((2,) * (grp_bits - 1 + tok_bits) + (rows // 2, piece))
        for axis, mask, dim in steps:
            part = fold(part.astype(jnp.bfloat16), axis, mask, dim)
        done.append(part.reshape(rows // 2, piece))
    return (jnp.concatenate(done, 0) / samples).astype(jnp.bfloat16)


def solution(mesh):
    placed = (
        P("shard", None),
        P("shard", None),
        P("shard", None),
        P(None, "shard", None),
        P(None, "shard"),
        P(None, "shard"),
        P(None, None, "shard"),
        P("grp", "shard", None),
        P("grp", None, "shard"),
        P("grp", None),
    )
    return jax.shard_map(
        body, mesh=mesh, in_specs=placed, out_specs=P("shard", "grp"), check_vma=False
    )
```

```python
import functools
import math

import jax
import jax.numpy as jnp
from jax import lax
from jax.experimental import pallas as pl
from jax.experimental.pallas import tpu as pltpu
from jax.sharding import PartitionSpec as P

UNIT = 32


def from_partner(value, axis, mask):
    pairs = [(source, source ^ mask) for source in range(lax.axis_size(axis))]
    return lax.ppermute(value, axis, pairs)


def sample_kernel(scale, unit, order_ref, spread_ref, mean_ref, variance_ref, deviation_ref, noise_ref, out_ref):
    samples = noise_ref.shape[0]
    columns, rows, width = deviation_ref.shape

    def step(i, carry):
        at = pl.ds(pl.multiple_of(i * unit, unit), unit)
        stacked = deviation_ref[:, at, :].reshape(columns * unit, width)
        low_rank = jnp.dot(spread_ref[...], stacked, preferred_element_type=jnp.float32)
        mean = mean_ref[at, :]
        std = jnp.sqrt(variance_ref[at, :])
        for s in range(samples):
            part = low_rank[s * unit : (s + 1) * unit]
            value = mean + std * noise_ref[s, at, :].astype(jnp.float32) + part * scale
            out_ref[s, at, :] = value.astype(out_ref.dtype)
        return carry

    lax.fori_loop(0, rows // unit, step, 0)


def sample_weights(order, parts, mean, variance, deviation, noise, low_half, name):
    columns, rows, width = deviation.shape
    samples = noise.shape[0]
    per_part = rows // parts
    unit = math.gcd(UNIT, per_part)
    block = max(
        b
        for b in range(unit, per_part + 1, unit)
        if per_part % b == 0 and (b == unit or columns * b * width * 2 <= 4500000)
    )
    steps = per_part // block
    eye = jnp.eye(unit, dtype=jnp.bfloat16)
    spread = (low_half[:, None, :, None] * eye[None, :, None, :]).reshape(samples * unit, columns * unit)

    def source(i, order):
        return order[i // steps] * steps + i % steps

    count = rows * width
    return pl.pallas_call(
        functools.partial(sample_kernel, 1.0 / math.sqrt(2.0 * (columns - 1)), unit),
        grid_spec=pltpu.PrefetchScalarGridSpec(
            num_scalar_prefetch=1,
            grid=(parts * steps,),
            in_specs=[
                pl.BlockSpec(spread.shape, lambda i, o: (0, 0)),
                pl.BlockSpec((block, width), lambda i, o: (source(i, o), 0)),
                pl.BlockSpec((block, width), lambda i, o: (source(i, o), 0)),
                pl.BlockSpec((columns, block, width), lambda i, o: (0, source(i, o), 0)),
                pl.BlockSpec((samples, block, width), lambda i, o: (0, source(i, o), 0)),
            ],
            out_specs=pl.BlockSpec((samples, block, width), lambda i, o: (0, i, 0)),
        ),
        out_shape=jax.ShapeDtypeStruct((samples, rows, width), jnp.bfloat16),
        cost_estimate=pl.CostEstimate(
            flops=2 * count * columns * samples,
            bytes_accessed=count * (2 * columns + 8 + 4 * samples),
            transcendentals=count,
        ),
        compiler_params=pltpu.CompilerParams(
            dimension_semantics=("arbitrary",), vmem_limit_bytes=60 * 1024 * 1024
        ),
        name=name,
    )(order, spread, mean, variance, deviation, noise)


def mlp_kernel(rows, core_ref, own_ref, other_ref, up_ref, down_ref, *out_refs):
    half = own_ref.shape[1]
    pairs, kept, piece = out_refs[0].shape
    core = core_ref[0]
    own_at = pl.ds(pl.multiple_of(core * half, half), half)
    other_at = pl.ds(pl.multiple_of((1 - core) * half, half), half)
    across = (((1,), (1,)), ((), ()))
    total = None
    for s in range(up_ref.shape[0]):
        preact = lax.dot_general(own_ref[...], up_ref[s, :, own_at], across, preferred_element_type=jnp.float32)
        preact += lax.dot_general(other_ref[...], up_ref[s, :, other_at], across, preferred_element_type=jnp.float32)
        hidden = (0.5 * preact * (1.0 + lax.erf(preact * math.sqrt(0.5)))).astype(jnp.bfloat16)
        term = lax.dot_general(hidden, down_ref[s], across, preferred_element_type=jnp.float32)
        total = term if total is None else total + term
    for p in range(2 * pairs):
        part = total[:, p * piece : (p + 1) * piece].astype(out_refs[0].dtype)
        part = part.reshape(2 * kept // rows, 2, rows // 2, piece)
        for stream in range(2):
            out_refs[2 * (p % 2) + stream][p // 2] = part[:, stream].reshape(kept, piece)


def mlp(core, own, other, up, down, parts, rows):
    tokens, half = own.shape
    samples, hidden, width = up.shape
    block = min(tokens, rows * max(1, 256 // rows))
    piece = width // parts
    return pl.pallas_call(
        functools.partial(mlp_kernel, rows),
        grid_spec=pltpu.PrefetchScalarGridSpec(
            num_scalar_prefetch=1,
            grid=(tokens // block,),
            in_specs=[
                pl.BlockSpec((block, half), lambda i, c: (i, 0)),
                pl.BlockSpec((block, half), lambda i, c: (i, 0)),
                pl.BlockSpec(up.shape, lambda i, c: (0, 0, 0)),
                pl.BlockSpec(down.shape, lambda i, c: (0, 0, 0)),
            ],
            out_specs=[pl.BlockSpec((parts // 2, block // 2, piece), lambda i, c: (0, i, 0))] * 4,
        ),
        out_shape=[jax.ShapeDtypeStruct((parts // 2, tokens // 2, piece), jnp.bfloat16)] * 4,
        cost_estimate=pl.CostEstimate(
            flops=4 * tokens * samples * hidden * width,
            bytes_accessed=2 * (2 * tokens * width + 2 * samples * hidden * width),
            transcendentals=tokens * samples * hidden,
        ),
        compiler_params=pltpu.CompilerParams(
            dimension_semantics=("arbitrary",), vmem_limit_bytes=60 * 1024 * 1024
        ),
        name="mlp",
    )(core, own, other, up, down)


def fold(value, axis, mask, dim):
    kept = lax.index_in_dim(value, 0, dim, keepdims=True)
    sent = lax.index_in_dim(value, 1, dim, keepdims=True).astype(jnp.bfloat16)
    return kept.astype(jnp.float32) + from_partner(sent, axis, mask).astype(jnp.float32)


MESH_ID = pl.DeviceIdType.MESH
SLOTS = 8
PRE_PARTS = 2
POST_PARTS = 1


def fused_kernel(
    cfg,
    low_ref,
    tokens_ref,
    mean1_ref,
    var1_ref,
    dev1_ref,
    mean2_ref,
    var2_ref,
    dev2_ref,
    noise1_ref,
    noise2_ref,
    out_ref,
    lowbuf,
    spread4,
    spread2,
    tok,
    dbuf1,
    mbuf1,
    nz1,
    up,
    dbuf2,
    mbuf2,
    nz2,
    down,
    hid,
    part,
    s1send,
    s1recv,
    s2send,
    s2keep,
    s2recv,
    s3send,
    s3recv,
    fin,
    sem_ld1,
    sem_ld2,
    sem_tok,
    sem_low,
    sem_n1,
    sem_n2,
    sem_z,
    sem_y,
    sem_x,
    sem_d,
    sem_h,
    sem_s1,
    sem_s2,
    sem_s3,
):
    unit, main, mid, rows2, scale, total_samples = cfg
    columns = dev1_ref.shape[0]
    hidden = dev1_ref.shape[1]
    width = dev1_ref.shape[2]
    own_samples = noise1_ref.shape[0]
    samples = 2 * own_samples
    block, _ = tokens_ref.shape
    half = width // 2
    piece = out_ref.shape[0]
    n_mid, n_main = mid // unit, main // unit
    n1 = n_mid + n_main
    n2 = 2 * piece // rows2
    steps = lax.axis_size("shard") // 2

    g = lax.axis_index("grp")
    s = lax.axis_index("shard")
    c = g % 2
    x = g // 2
    y = s % 2
    z = s // 2
    partner = (g ^ 1, s)
    xn = (g ^ 2, s)
    yn = (g, s ^ 1)
    first_peer = (g ^ (2 * (1 - c)), s ^ c)
    second_peer = (g ^ (2 * c), s ^ (1 - c))

    def zn(k):
        return (g, s ^ (2 * k))

    def remote(src, dst, sems, index, device):
        return pltpu.make_async_remote_copy(
            src_ref=src,
            dst_ref=dst,
            send_sem=sems.at[(0,) + index],
            recv_sem=sems.at[(1,) + index],
            device_id=device,
            device_id_type=MESH_ID,
        )

    def copies1(i):
        slot = i % SLOTS
        at_mid = i < n_mid
        row = pl.multiple_of(jnp.where(at_mid, main + i * unit, c * (main + mid) + (i - n_mid) * unit), unit)
        place = pl.multiple_of(jnp.where(at_mid, main + i * unit, (i - n_mid) * unit), unit)
        src = pl.ds(row, unit)
        own = pl.ds(own_samples * c, own_samples)
        return (
            pltpu.make_async_copy(dev1_ref.at[:, src, :], dbuf1.at[slot], sem_ld1.at[slot, 0]),
            pltpu.make_async_copy(mean1_ref.at[src, :], mbuf1.at[slot, 0], sem_ld1.at[slot, 1]),
            pltpu.make_async_copy(var1_ref.at[src, :], mbuf1.at[slot, 1], sem_ld1.at[slot, 2]),
            pltpu.make_async_copy(noise1_ref.at[:, src, :], nz1.at[own, pl.ds(place, unit), :], sem_ld1.at[slot, 3]),
        )

    def feature_row(core, j):
        per = n2 // 2
        first = j < per
        chip = jnp.where(first, 1 - x, x)
        inner = jnp.where(first, j, j - per)
        return pl.multiple_of(chip * 2 * piece + core * piece + inner * rows2, math.gcd(piece, rows2))

    def copies2(j):
        slot = j % SLOTS
        src = pl.ds(feature_row(c, j), rows2)
        own = pl.ds(own_samples * c, own_samples)
        to = pl.ds(pl.multiple_of(j * rows2, rows2), rows2)
        return (
            pltpu.make_async_copy(dev2_ref.at[:, src, :], dbuf2.at[slot], sem_ld2.at[slot, 0]),
            pltpu.make_async_copy(mean2_ref.at[src, :], mbuf2.at[slot, 0], sem_ld2.at[slot, 1]),
            pltpu.make_async_copy(var2_ref.at[src, :], mbuf2.at[slot, 1], sem_ld2.at[slot, 2]),
            pltpu.make_async_copy(noise2_ref.at[:, src, :], nz2.at[own, to, :], sem_ld2.at[slot, 3]),
        )

    def start(copies):
        for copy in copies:
            copy.start()

    def wait(copies):
        for copy in copies:
            copy.wait()

    own_tokens = pltpu.make_async_copy(tokens_ref, tok.at[s], sem_tok)
    own_tokens.start()
    barrier = pltpu.get_barrier_semaphore()
    peers = [partner, xn, yn] + [zn(k) for k in range(1, steps)]
    for peer in peers:
        pl.semaphore_signal(barrier, inc=1, device_id=peer, device_id_type=MESH_ID)

    def start_later(q):
        @pl.when(q < n1)
        def _():
            start(copies1(q))

        @pl.when(jnp.logical_and(q >= n1, q < n1 + n2))
        def _():
            start(copies2(q - n1))

    def spread_of(low):
        count = low.shape[0]
        pick = lax.broadcasted_iota(jnp.int32, (columns, columns * unit), 1) // unit
        pick = (pick == lax.broadcasted_iota(jnp.int32, (columns, columns * unit), 0)).astype(jnp.bfloat16)
        wide = jnp.dot(low.astype(jnp.bfloat16), pick, preferred_element_type=jnp.float32)
        lane = lax.broadcasted_iota(jnp.int32, (unit, columns * unit), 1) % unit
        eye = lane == lax.broadcasted_iota(jnp.int32, (unit, columns * unit), 0)
        parts = [jnp.where(eye, wide[i : i + 1, :], 0.0) for i in range(count)]
        return [p.astype(jnp.bfloat16) for p in parts]

    own_tokens.wait()
    for i in range(min(SLOTS, n1)):
        start(copies1(jnp.int32(i)))
    mine = spread_of(low_ref[...])
    for i in range(own_samples):
        spread2[pl.ds(i * unit, unit), :] = mine[i]

    def mid_step(i, carry):
        slot = i % SLOTS
        wait(copies1(i))
        stacked = dbuf1[slot].reshape(columns * unit, width)
        low_rank = jnp.dot(spread2[...], stacked, preferred_element_type=jnp.float32)
        mean = mbuf1[slot, 0]
        std = jnp.sqrt(mbuf1[slot, 1])
        from_row = pl.ds(pl.multiple_of(main + i * unit, unit), unit)
        for n in range(own_samples):
            noise = nz1[own_samples * c + n, from_row, :].astype(jnp.float32)
            value = mean + std * noise + low_rank[n * unit : (n + 1) * unit] * scale
            to = pl.ds(pl.multiple_of(samples * main + n * mid + i * unit, unit), unit)
            up[to, :] = value.astype(up.dtype)
        start_later(i + SLOTS)
        return carry

    lax.fori_loop(0, n_mid, mid_step, 0)

    pl.semaphore_wait(barrier, len(peers))

    lanes = pl.ds(pl.multiple_of(c * half, half), half)

    def low_copy():
        return remote(low_ref, lowbuf, sem_low, (), partner)

    def noise1_copy(i):
        src = pl.ds(pl.multiple_of((1 - c) * (main + mid) + i * unit, unit), unit)
        to = pl.ds(pl.multiple_of(i * unit, unit), unit)
        own = pl.ds(own_samples * c, own_samples)
        return remote(noise1_ref.at[:, src, :], nz1.at[own, to, :], sem_n1, (i,), partner)

    def noise1_arrival(i):
        src = pl.ds(pl.multiple_of((1 - c) * (main + mid) + i * unit, unit), unit)
        to = pl.ds(pl.multiple_of(i * unit, unit), unit)
        other = pl.ds(own_samples * (1 - c), own_samples)
        return remote(noise1_ref.at[:, src, :], nz1.at[other, to, :], sem_n1, (i,), partner)

    def noise2_copy(j):
        src = pl.ds(feature_row(1 - c, j), rows2)
        to = pl.ds(pl.multiple_of(j * rows2, rows2), rows2)
        own = pl.ds(own_samples * c, own_samples)
        return remote(noise2_ref.at[:, src, :], nz2.at[own, to, :], sem_n2, (j,), partner)

    def noise2_arrival(j):
        src = pl.ds(feature_row(1 - c, j), rows2)
        to = pl.ds(pl.multiple_of(j * rows2, rows2), rows2)
        other = pl.ds(own_samples * (1 - c), own_samples)
        return remote(noise2_ref.at[:, src, :], nz2.at[other, to, :], sem_n2, (j,), partner)

    def token_copy(shard, sems, index, device):
        ref = tok.at[shard, :, lanes]
        return remote(ref, ref, sems, index, device)

    own_rows = pl.ds(pl.multiple_of(x * (block // 2), block // 2), block // 2)
    other_rows = pl.ds(pl.multiple_of((1 - x) * (block // 2), block // 2), block // 2)

    def part_copy(shard, rows, sems, index, device):
        ref = tok.at[shard, rows, lanes]
        return remote(ref, ref, sems, index, device)

    def z_copy(k):
        if k == 1:
            return token_copy(s, sem_z, (k,), zn(k))
        return part_copy(s, own_rows, sem_z, (k,), zn(k))

    def z_arrival(k):
        if k == 1:
            return token_copy(s ^ 2, sem_z, (k,), zn(k))
        return part_copy(s ^ (2 * k), own_rows, sem_z, (k,), zn(k))

    def forward_copy():
        return part_copy(s ^ 4, own_rows, sem_z, (3,), zn(1))

    def y_copy(k):
        if k < 2:
            return token_copy(s ^ (2 * k), sem_y, (k,), yn)
        return part_copy(s ^ (2 * k), own_rows, sem_y, (k,), yn)

    def y_arrival(k):
        if k < 2:
            return token_copy(s ^ (2 * k) ^ 1, sem_y, (k,), yn)
        return part_copy(s ^ (2 * k) ^ 1, own_rows, sem_y, (k,), yn)

    def x_copy(k, side):
        return part_copy(s ^ (2 * k) ^ side, own_rows, sem_x, (k, side), xn)

    def x_arrival(k, side):
        return part_copy(s ^ (2 * k) ^ side, other_rows, sem_x, (k, side), xn)

    def d_copy(k, side):
        return token_copy(s ^ (2 * k) ^ side, sem_d, (k, side), partner)

    def d_arrival(k, side):
        other = pl.ds(pl.multiple_of((1 - c) * half, half), half)
        ref = tok.at[s ^ (2 * k) ^ side, :, other]
        return remote(ref, ref, sem_d, (k, side), partner)

    low_copy().start()
    y_copy(0).start()

    z_copy(2).start()
    z_copy(1).start()
    for i in range(n_main):
        noise1_copy(i).start()

    low_copy().wait_recv()
    others = spread_of(lowbuf[...])
    for i in range(own_samples):
        first = c == 0
        spread4[pl.ds(i * unit, unit), :] = jnp.where(first, mine[i], others[i])
        spread4[pl.ds((own_samples + i) * unit, unit), :] = jnp.where(first, others[i], mine[i])

    def main_step(i, carry):
        q = i + n_mid
        slot = q % SLOTS
        wait(copies1(q))
        noise1_arrival(i).wait_recv()
        stacked = dbuf1[slot].reshape(columns * unit, width)
        low_rank = jnp.dot(spread4[...], stacked, preferred_element_type=jnp.float32)
        mean = mbuf1[slot, 0]
        std = jnp.sqrt(mbuf1[slot, 1])
        from_row = pl.ds(pl.multiple_of(i * unit, unit), unit)
        for n in range(samples):
            noise = nz1[n, from_row, :].astype(jnp.float32)
            value = mean + std * noise + low_rank[n * unit : (n + 1) * unit] * scale
            up[pl.ds(pl.multiple_of(n * main + i * unit, unit), unit), :] = value.astype(up.dtype)
        start_later(q + SLOTS)
        noise2_copy(i).start()
        return carry

    def down_step(j, carry):
        slot = j % SLOTS
        wait(copies2(j))
        noise2_arrival(j).wait_recv()
        per_core = samples * main + own_samples * mid
        for u in range(rows2 // unit):
            inner = pl.ds(u * unit, unit)
            at = pl.ds(pl.multiple_of(j * rows2 + u * unit, unit), unit)
            stacked = dbuf2[slot, :, inner, :].reshape(columns * unit, hidden)
            low_rank = jnp.dot(spread4[...], stacked, preferred_element_type=jnp.float32)
            mean = mbuf2[slot, 0, inner, :]
            std = jnp.sqrt(mbuf2[slot, 1, inner, :])
            for n in range(samples):
                noise = nz2[n, at, :].astype(jnp.float32)
                value = mean + std * noise + low_rank[n * unit : (n + 1) * unit] * scale
                value = value.astype(down.dtype)
                holder, local = n // own_samples, n % own_samples
                down[at, pl.ds(n * main, main)] = value[:, :main]
                down[at, pl.ds(per_core + n * main, main)] = value[:, main + mid :]
                down[at, pl.ds(holder * per_core + samples * main + local * mid, mid)] = value[:, main : main + mid]
        start_later(n1 + j + SLOTS)
        return carry

    def hidden_copy(k):
        ref = hid.at[k, c]
        return remote(ref, ref, sem_h, (k,), partner)

    def hidden_arrival(k):
        ref = hid.at[k, 1 - c]
        return remote(ref, ref, sem_h, (k,), partner)

    across = (((1,), (1,)), ((), ()))

    def pre(k):
        zz = z ^ k
        if k:
            d_arrival(k, 0).wait_recv()
        d_arrival(k, 1).wait_recv()
        held = tok[pl.ds(2 * zz, 2), :, :].reshape(2 * block, width)

        size = hid.shape[2] // PRE_PARTS

        def rows_step(n, carry):
            at = pl.ds(pl.multiple_of(n * size, size), size)
            preact = lax.dot_general(up[at, :], held, across, preferred_element_type=jnp.float32)
            value = 0.5 * preact * (1.0 + lax.erf(preact * math.sqrt(0.5)))
            hid[k, c, at, :] = value.astype(hid.dtype)
            return carry

        lax.fori_loop(0, PRE_PARTS, rows_step, 0)
        hidden_copy(k).start()

    onward = jnp.where(c == 0, 1 - y, 0)

    def s1_copy(k, i):
        return remote(s1send.at[k, i], s1recv.at[k, i], sem_s1, (k, i), first_peer)

    def s2_copy(k):
        return remote(s2send.at[k], s2recv.at[k], sem_s2, (k,), second_peer)

    def s3_copy(k):
        return remote(s3send.at[k], s3recv.at[k], sem_s3, (k,), zn(k))

    def post(k):
        hidden_arrival(k).wait_recv()
        held = hid[k].reshape(down.shape[1], 2 * block)
        size = piece // POST_PARTS

        def rows_step(n, carry):
            kept, inner = n // POST_PARTS, n % POST_PARTS
            at = pl.ds(pl.multiple_of(n * size, size), size)
            to = pl.ds(pl.multiple_of(inner * size, size), size)
            total = jnp.dot(down[at, :], held, preferred_element_type=jnp.float32)
            for side in range(2):
                part[k, kept, side, to, :] = total[:, side * block : (side + 1) * block]
            return carry

        lax.fori_loop(0, 2 * POST_PARTS, rows_step, 0)
        for i in (onward, 1 - onward):
            value = part[k, jnp.where(c == 0, 0, i), jnp.where(c == 0, i, 1 - y)]
            s1send[k, i] = value.astype(s1send.dtype)
            s1_copy(k, i).start()

    def summed(k, i):
        s1_copy(k, i).wait_recv()
        value = part[k, jnp.where(c == 0, 1, i), jnp.where(c == 0, i, y)]
        return value + s1recv[k, i].astype(jnp.float32)

    def stage2(k):
        s2send[k] = summed(k, onward).astype(s2send.dtype)
        s2_copy(k).start()
        s2keep[k] = summed(k, 1 - onward)

    def stage3(k):
        s2_copy(k).wait_recv()
        value = s2keep[k] + s2recv[k].astype(jnp.float32)
        if k == 0:
            fin[...] = value
        else:
            s3send[k] = value.astype(s3send.dtype)
            s3_copy(k).start()

    def far_z(k):
        z_arrival(k).wait_recv()
        if k == 2:
            forward_copy().start()
        y_copy(k).start()
        x_copy(k, 0).start()

    def far_y(k):
        y_arrival(k).wait_recv()
        x_copy(k, 1).start()

    def far_x(k, side):
        x_arrival(k, side).wait_recv()
        d_copy(k, side).start()

    def near_z():
        z_arrival(1).wait_recv()
        d_copy(1, 0).start()

    def near_y(k):
        y_arrival(k).wait_recv()
        d_copy(k, 1).start()

    def sample_down(first, last):
        lax.fori_loop(first * n2 // 10, last * n2 // 10, down_step, 0)

    lax.fori_loop(0, n_main, main_step, 0)
    for j in range(n_main, n2):
        noise2_copy(j).start()
    sample_down(0, 2)
    far_z(2)
    near_y(0)
    sample_down(2, 4)
    near_z()
    sample_down(4, 6)
    far_z(3)
    y_copy(1).start()
    far_x(2, 0)
    far_y(2)
    pre(0)
    sample_down(6, 10)
    far_x(3, 0)
    far_y(3)
    far_x(2, 1)
    post(0)
    near_y(1)
    pre(2)
    far_x(3, 1)
    pre(1)
    post(2)
    stage2(0)
    pre(3)
    post(1)
    post(3)
    stage2(2)
    stage3(0)
    stage2(1)
    stage3(2)
    stage2(3)
    stage3(1)
    stage3(3)
    result = fin[...]
    for k in range(1, steps):
        s3_copy(k).wait_recv()
        result = result + s3recv[k].astype(jnp.float32)
    result = result / total_samples
    out_ref[...] = result.astype(out_ref.dtype)

    low_copy().wait_send()
    for i in range(n_main):
        noise1_copy(i).wait_send()
    for j in range(n2):
        noise2_copy(j).wait_send()
    z_copy(1).wait_send()

    z_copy(2).wait_send()
    forward_copy().wait_send()
    for k in range(steps):
        y_copy(k).wait_send()
        d_copy(k, 1).wait_send()
        hidden_copy(k).wait_send()
        s1_copy(k, 0).wait_send()
        s1_copy(k, 1).wait_send()
        s2_copy(k).wait_send()
        if k:
            d_copy(k, 0).wait_send()
            s3_copy(k).wait_send()
        if k > 1:
            x_copy(k, 0).wait_send()
            x_copy(k, 1).wait_send()


def fused(
    tokens,
    fc1_mean,
    fc1_variance,
    fc1_deviation,
    fc2_mean,
    fc2_variance,
    fc2_deviation,
    noise_fc1,
    noise_fc2,
    noise_low,
):
    columns, hidden, width = fc1_deviation.shape
    own = noise_fc1.shape[0]
    samples = 2 * own
    groups = lax.axis_size("grp")
    shards = lax.axis_size("shard")
    steps = shards // 2
    block = tokens.shape[0]
    piece = width // groups
    tiles = hidden // 128
    main = tiles // 2 * 128
    mid = hidden - 2 * main
    unit = UNIT
    rows2 = 2 * unit
    n_main = main // unit
    n2 = 2 * piece // rows2
    per_core = samples * main + own * mid
    cfg = (unit, main, mid, rows2, 1.0 / math.sqrt(2.0 * (columns - 1)), own * groups)
    hbm = pl.BlockSpec(memory_space=pltpu.HBM)
    vmem = pl.BlockSpec(memory_space=pltpu.VMEM)
    bf16, f32 = jnp.bfloat16, jnp.float32
    dma = pltpu.SemaphoreType.DMA
    return pl.pallas_call(
        functools.partial(fused_kernel, cfg),
        out_shape=jax.ShapeDtypeStruct((piece, block), bf16),
        in_specs=[vmem] + [hbm] * 9,
        out_specs=vmem,
        scratch_shapes=[
            pltpu.VMEM(noise_low.shape, f32),
            pltpu.VMEM((samples * unit, columns * unit), bf16),
            pltpu.VMEM((own * unit, columns * unit), bf16),
            pltpu.VMEM((shards, block, width), bf16),
            pltpu.VMEM((SLOTS, columns, unit, width), bf16),
            pltpu.VMEM((SLOTS, 2, unit, width), f32),
            pltpu.VMEM((samples, main + mid, width), bf16),
            pltpu.VMEM((per_core, width), bf16),
            pltpu.VMEM((SLOTS, columns, rows2, hidden), bf16),
            pltpu.VMEM((SLOTS, 2, rows2, hidden), f32),
            pltpu.VMEM((samples, 2 * piece, hidden), bf16),
            pltpu.VMEM((2 * piece, 2 * per_core), bf16),
            pltpu.VMEM((steps, 2, per_core, 2 * block), bf16),
            pltpu.VMEM((steps, 2, 2, piece, block), f32),
            pltpu.VMEM((steps, 2, piece, block), bf16),
            pltpu.VMEM((steps, 2, piece, block), bf16),
            pltpu.VMEM((steps, piece, block), bf16),
            pltpu.VMEM((steps, piece, block), f32),
            pltpu.VMEM((steps, piece, block), bf16),
            pltpu.VMEM((steps, piece, block), bf16),
            pltpu.VMEM((steps, piece, block), bf16),
            pltpu.VMEM((piece, block), f32),
            dma((SLOTS, 4)),
            dma((SLOTS, 4)),
            dma,
            dma((2,)),
            dma((2, n_main)),
            dma((2, n2)),
            dma((2, steps)),
            dma((2, steps)),
            dma((2, steps, 2)),
            dma((2, steps, 2)),
            dma((2, steps)),
            dma((2, steps, 2)),
            dma((2, steps)),
            dma((2, steps)),
        ],
        compiler_params=pltpu.CompilerParams(
            collective_id=0, has_side_effects=True, vmem_limit_bytes=67043328
        ),
        name="swag",
    )(
        noise_low,
        tokens,
        fc1_mean,
        fc1_variance,
        fc1_deviation,
        fc2_mean,
        fc2_variance,
        fc2_deviation,
        noise_fc1,
        noise_fc2,
    ).T


def fits_fused(groups, shards, tokens, deviation):
    width, hidden = tokens.shape[1], deviation.shape[1]
    return (
        groups == 4
        and shards == 8
        and hidden % 128 == 0
        and hidden // 128 % 2 == 1
        and width % 256 == 0
        and width // groups % (2 * UNIT) == 0
        and tokens.shape[0] % 128 == 0
    )


def body(
    tokens,
    fc1_mean,
    fc1_variance,
    fc1_deviation,
    fc2_mean,
    fc2_variance,
    fc2_deviation,
    noise_fc1,
    noise_fc2,
    noise_low,
):
    groups = lax.axis_size("grp")
    shard_count = lax.axis_size("shard")
    if fits_fused(groups, shard_count, tokens, fc1_deviation):
        return fused(
            tokens,
            fc1_mean,
            fc1_variance,
            fc1_deviation,
            fc2_mean,
            fc2_variance,
            fc2_deviation,
            noise_fc1,
            noise_fc2,
            noise_low,
        )
    low_half = noise_low.astype(jnp.bfloat16)
    samples = noise_fc1.shape[0] * groups
    hid_ways = min(8, shard_count)
    low_bits = (shard_count // hid_ways).bit_length() - 1
    tok_bits = hid_ways.bit_length() - 1
    grp_bits = groups.bit_length() - 1
    position = lax.axis_index("shard")
    group = lax.axis_index("grp")
    core = group % 2
    rows, width = tokens.shape
    half = width // 2

    mine = lax.dynamic_slice_in_dim(tokens, core * half, half, 1)
    gathered = [mine] + [from_partner(mine, "shard", m << low_bits) for m in range(1, hid_ways)]

    order = jnp.bitwise_xor(jnp.arange(groups, dtype=jnp.int32), group.astype(jnp.int32))
    whole = jnp.zeros((1,), jnp.int32)
    up = sample_weights(whole, 1, fc1_mean, fc1_variance, fc1_deviation, noise_fc1, low_half, "sample_up")
    down = sample_weights(order, groups, fc2_mean, fc2_variance, fc2_deviation, noise_fc2, low_half, "sample_down")
    for bit in range(low_bits):
        upper = position >> bit & 1 == 1
        partner = from_partner(up, "shard", 1 << bit)
        up = jnp.where(upper, jnp.concatenate([partner, up], 1), jnp.concatenate([up, partner], 1))
        partner = from_partner(down, "shard", 1 << bit)
        down = jnp.where(upper, jnp.concatenate([partner, down], 2), jnp.concatenate([down, partner], 2))

    gathered, up, down = lax.optimization_barrier((gathered, up, down))
    own = jnp.concatenate(gathered, 0)
    other = from_partner(own, "grp", 1)
    piece = width // groups
    kept_and_sent = mlp(core.astype(jnp.int32).reshape(1), own, other, up, down, groups, rows)
    grp_steps = [("grp", 1 << b, grp_bits - 1 - b) for b in range(1, grp_bits)]
    shard_steps = [("shard", 1 << (low_bits + b), grp_bits + tok_bits - 2 - b) for b in range(tok_bits)]
    first, second, rest = grp_steps, shard_steps[:1], shard_steps[:0:-1]
    done = []
    for stream, steps in enumerate((first + second + rest, second + first + rest)):
        swapped = from_partner(kept_and_sent[2 + stream], "grp", 1)
        part = kept_and_sent[stream].astype(jnp.float32) + swapped.astype(jnp.float32)
        part = part.reshape((2,) * (grp_bits - 1 + tok_bits) + (rows // 2, piece))
        for axis, mask, dim in steps:
            part = fold(part.astype(jnp.bfloat16), axis, mask, dim)
        done.append(part.reshape(rows // 2, piece))
    return (jnp.concatenate(done, 0) / samples).astype(jnp.bfloat16)


def solution(mesh):
    placed = (
        P("shard", None),
        P("shard", None),
        P("shard", None),
        P(None, "shard", None),
        P(None, "shard"),
        P(None, "shard"),
        P(None, None, "shard"),
        P("grp", "shard", None),
        P("grp", None, "shard"),
        P("grp", None),
    )
    return jax.shard_map(
        body, mesh=mesh, in_specs=placed, out_specs=P("shard", "grp"), check_vma=False
    )
```

```python
import functools
import math

import jax
import jax.numpy as jnp
from jax import lax
from jax.experimental import pallas as pl
from jax.experimental.pallas import tpu as pltpu
from jax.sharding import PartitionSpec as P

UNIT = 32


def from_partner(value, axis, mask):
    pairs = [(source, source ^ mask) for source in range(lax.axis_size(axis))]
    return lax.ppermute(value, axis, pairs)


def sample_kernel(scale, unit, order_ref, spread_ref, mean_ref, variance_ref, deviation_ref, noise_ref, out_ref):
    samples = noise_ref.shape[0]
    columns, rows, width = deviation_ref.shape

    def step(i, carry):
        at = pl.ds(pl.multiple_of(i * unit, unit), unit)
        stacked = deviation_ref[:, at, :].reshape(columns * unit, width)
        low_rank = jnp.dot(spread_ref[...], stacked, preferred_element_type=jnp.float32)
        mean = mean_ref[at, :]
        std = jnp.sqrt(variance_ref[at, :])
        for s in range(samples):
            part = low_rank[s * unit : (s + 1) * unit]
            value = mean + std * noise_ref[s, at, :].astype(jnp.float32) + part * scale
            out_ref[s, at, :] = value.astype(out_ref.dtype)
        return carry

    lax.fori_loop(0, rows // unit, step, 0)


def sample_weights(order, parts, mean, variance, deviation, noise, low_half, name):
    columns, rows, width = deviation.shape
    samples = noise.shape[0]
    per_part = rows // parts
    unit = math.gcd(UNIT, per_part)
    block = max(
        b
        for b in range(unit, per_part + 1, unit)
        if per_part % b == 0 and (b == unit or columns * b * width * 2 <= 4500000)
    )
    steps = per_part // block
    eye = jnp.eye(unit, dtype=jnp.bfloat16)
    spread = (low_half[:, None, :, None] * eye[None, :, None, :]).reshape(samples * unit, columns * unit)

    def source(i, order):
        return order[i // steps] * steps + i % steps

    count = rows * width
    return pl.pallas_call(
        functools.partial(sample_kernel, 1.0 / math.sqrt(2.0 * (columns - 1)), unit),
        grid_spec=pltpu.PrefetchScalarGridSpec(
            num_scalar_prefetch=1,
            grid=(parts * steps,),
            in_specs=[
                pl.BlockSpec(spread.shape, lambda i, o: (0, 0)),
                pl.BlockSpec((block, width), lambda i, o: (source(i, o), 0)),
                pl.BlockSpec((block, width), lambda i, o: (source(i, o), 0)),
                pl.BlockSpec((columns, block, width), lambda i, o: (0, source(i, o), 0)),
                pl.BlockSpec((samples, block, width), lambda i, o: (0, source(i, o), 0)),
            ],
            out_specs=pl.BlockSpec((samples, block, width), lambda i, o: (0, i, 0)),
        ),
        out_shape=jax.ShapeDtypeStruct((samples, rows, width), jnp.bfloat16),
        cost_estimate=pl.CostEstimate(
            flops=2 * count * columns * samples,
            bytes_accessed=count * (2 * columns + 8 + 4 * samples),
            transcendentals=count,
        ),
        compiler_params=pltpu.CompilerParams(
            dimension_semantics=("arbitrary",), vmem_limit_bytes=60 * 1024 * 1024
        ),
        name=name,
    )(order, spread, mean, variance, deviation, noise)


def mlp_kernel(rows, core_ref, own_ref, other_ref, up_ref, down_ref, *out_refs):
    half = own_ref.shape[1]
    pairs, kept, piece = out_refs[0].shape
    core = core_ref[0]
    own_at = pl.ds(pl.multiple_of(core * half, half), half)
    other_at = pl.ds(pl.multiple_of((1 - core) * half, half), half)
    across = (((1,), (1,)), ((), ()))
    total = None
    for s in range(up_ref.shape[0]):
        preact = lax.dot_general(own_ref[...], up_ref[s, :, own_at], across, preferred_element_type=jnp.float32)
        preact += lax.dot_general(other_ref[...], up_ref[s, :, other_at], across, preferred_element_type=jnp.float32)
        hidden = (0.5 * preact * (1.0 + lax.erf(preact * math.sqrt(0.5)))).astype(jnp.bfloat16)
        term = lax.dot_general(hidden, down_ref[s], across, preferred_element_type=jnp.float32)
        total = term if total is None else total + term
    for p in range(2 * pairs):
        part = total[:, p * piece : (p + 1) * piece].astype(out_refs[0].dtype)
        part = part.reshape(2 * kept // rows, 2, rows // 2, piece)
        for stream in range(2):
            out_refs[2 * (p % 2) + stream][p // 2] = part[:, stream].reshape(kept, piece)


def mlp(core, own, other, up, down, parts, rows):
    tokens, half = own.shape
    samples, hidden, width = up.shape
    block = min(tokens, rows * max(1, 256 // rows))
    piece = width // parts
    return pl.pallas_call(
        functools.partial(mlp_kernel, rows),
        grid_spec=pltpu.PrefetchScalarGridSpec(
            num_scalar_prefetch=1,
            grid=(tokens // block,),
            in_specs=[
                pl.BlockSpec((block, half), lambda i, c: (i, 0)),
                pl.BlockSpec((block, half), lambda i, c: (i, 0)),
                pl.BlockSpec(up.shape, lambda i, c: (0, 0, 0)),
                pl.BlockSpec(down.shape, lambda i, c: (0, 0, 0)),
            ],
            out_specs=[pl.BlockSpec((parts // 2, block // 2, piece), lambda i, c: (0, i, 0))] * 4,
        ),
        out_shape=[jax.ShapeDtypeStruct((parts // 2, tokens // 2, piece), jnp.bfloat16)] * 4,
        cost_estimate=pl.CostEstimate(
            flops=4 * tokens * samples * hidden * width,
            bytes_accessed=2 * (2 * tokens * width + 2 * samples * hidden * width),
            transcendentals=tokens * samples * hidden,
        ),
        compiler_params=pltpu.CompilerParams(
            dimension_semantics=("arbitrary",), vmem_limit_bytes=60 * 1024 * 1024
        ),
        name="mlp",
    )(core, own, other, up, down)


def fold(value, axis, mask, dim):
    kept = lax.index_in_dim(value, 0, dim, keepdims=True)
    sent = lax.index_in_dim(value, 1, dim, keepdims=True).astype(jnp.bfloat16)
    return kept.astype(jnp.float32) + from_partner(sent, axis, mask).astype(jnp.float32)


MESH_ID = pl.DeviceIdType.MESH
SLOTS = 8
PRE_PARTS = 2
POST_PARTS = 1


def fused_kernel(
    cfg,
    low_ref,
    tokens_ref,
    mean1_ref,
    var1_ref,
    dev1_ref,
    mean2_ref,
    var2_ref,
    dev2_ref,
    noise1_ref,
    noise2_ref,
    out_ref,
    lowbuf,
    spread4,
    spread2,
    tok,
    dbuf1,
    mbuf1,
    nz1,
    up,
    dbuf2,
    mbuf2,
    nz2,
    down,
    hid,
    part,
    s1send,
    s1recv,
    s2send,
    s2keep,
    s2recv,
    s3send,
    s3recv,
    fin,
    sem_ld1,
    sem_ld2,
    sem_tok,
    sem_low,
    sem_n1,
    sem_n2,
    sem_z,
    sem_y,
    sem_x,
    sem_d,
    sem_h,
    sem_s1,
    sem_s2,
    sem_s3,
):
    unit, main, mid, rows2, scale, total_samples = cfg
    columns = dev1_ref.shape[0]
    hidden = dev1_ref.shape[1]
    width = dev1_ref.shape[2]
    own_samples = noise1_ref.shape[0]
    samples = 2 * own_samples
    block, _ = tokens_ref.shape
    half = width // 2
    piece = out_ref.shape[0]
    n_mid, n_main = mid // unit, main // unit
    n1 = n_mid + n_main
    n2 = 2 * piece // rows2
    steps = lax.axis_size("shard") // 2

    g = lax.axis_index("grp")
    s = lax.axis_index("shard")
    c = g % 2
    x = g // 2
    y = s % 2
    z = s // 2
    partner = (g ^ 1, s)
    xn = (g ^ 2, s)
    yn = (g, s ^ 1)
    first_peer = (g ^ (2 * (1 - c)), s ^ c)
    second_peer = (g ^ (2 * c), s ^ (1 - c))

    def zn(k):
        return (g, s ^ (2 * k))

    def remote(src, dst, sems, index, device):
        return pltpu.make_async_remote_copy(
            src_ref=src,
            dst_ref=dst,
            send_sem=sems.at[(0,) + index],
            recv_sem=sems.at[(1,) + index],
            device_id=device,
            device_id_type=MESH_ID,
        )

    def copies1(i):
        slot = i % SLOTS
        at_mid = i < n_mid
        row = pl.multiple_of(jnp.where(at_mid, main + i * unit, c * (main + mid) + (i - n_mid) * unit), unit)
        place = pl.multiple_of(jnp.where(at_mid, main + i * unit, (i - n_mid) * unit), unit)
        src = pl.ds(row, unit)
        own = pl.ds(own_samples * c, own_samples)
        return (
            pltpu.make_async_copy(dev1_ref.at[:, src, :], dbuf1.at[slot], sem_ld1.at[slot, 0]),
            pltpu.make_async_copy(mean1_ref.at[src, :], mbuf1.at[slot, 0], sem_ld1.at[slot, 1]),
            pltpu.make_async_copy(var1_ref.at[src, :], mbuf1.at[slot, 1], sem_ld1.at[slot, 2]),
            pltpu.make_async_copy(noise1_ref.at[:, src, :], nz1.at[own, pl.ds(place, unit), :], sem_ld1.at[slot, 3]),
        )

    def feature_row(core, j):
        per = n2 // 2
        first = j < per
        chip = jnp.where(first, 1 - x, x)
        inner = jnp.where(first, j, j - per)
        return pl.multiple_of(chip * 2 * piece + core * piece + inner * rows2, math.gcd(piece, rows2))

    def copies2(j):
        slot = j % SLOTS
        src = pl.ds(feature_row(c, j), rows2)
        own = pl.ds(own_samples * c, own_samples)
        to = pl.ds(pl.multiple_of(j * rows2, rows2), rows2)
        return (
            pltpu.make_async_copy(dev2_ref.at[:, src, :], dbuf2.at[slot], sem_ld2.at[slot, 0]),
            pltpu.make_async_copy(mean2_ref.at[src, :], mbuf2.at[slot, 0], sem_ld2.at[slot, 1]),
            pltpu.make_async_copy(var2_ref.at[src, :], mbuf2.at[slot, 1], sem_ld2.at[slot, 2]),
            pltpu.make_async_copy(noise2_ref.at[:, src, :], nz2.at[own, to, :], sem_ld2.at[slot, 3]),
        )

    def start(copies):
        for copy in copies:
            copy.start()

    def wait(copies):
        for copy in copies:
            copy.wait()

    own_tokens = pltpu.make_async_copy(tokens_ref, tok.at[s], sem_tok)
    own_tokens.start()
    barrier = pltpu.get_barrier_semaphore()
    peers = [partner, xn, yn] + [zn(k) for k in range(1, steps)]
    for peer in peers:
        pl.semaphore_signal(barrier, inc=1, device_id=peer, device_id_type=MESH_ID)

    def start_later(q):
        @pl.when(q < n1)
        def _():
            start(copies1(q))

        @pl.when(jnp.logical_and(q >= n1, q < n1 + n2))
        def _():
            start(copies2(q - n1))

    def spread_of(low):
        count = low.shape[0]
        pick = lax.broadcasted_iota(jnp.int32, (columns, columns * unit), 1) // unit
        pick = (pick == lax.broadcasted_iota(jnp.int32, (columns, columns * unit), 0)).astype(jnp.bfloat16)
        wide = jnp.dot(low.astype(jnp.bfloat16), pick, preferred_element_type=jnp.float32)
        lane = lax.broadcasted_iota(jnp.int32, (unit, columns * unit), 1) % unit
        eye = lane == lax.broadcasted_iota(jnp.int32, (unit, columns * unit), 0)
        parts = [jnp.where(eye, wide[i : i + 1, :], 0.0) for i in range(count)]
        return [p.astype(jnp.bfloat16) for p in parts]

    own_tokens.wait()
    for i in range(min(SLOTS, n1)):
        start(copies1(jnp.int32(i)))
    mine = spread_of(low_ref[...])
    for i in range(own_samples):
        spread2[pl.ds(i * unit, unit), :] = mine[i]

    def mid_step(i, carry):
        slot = i % SLOTS
        wait(copies1(i))
        stacked = dbuf1[slot].reshape(columns * unit, width)
        low_rank = jnp.dot(spread2[...], stacked, preferred_element_type=jnp.float32)
        mean = mbuf1[slot, 0]
        std = jnp.sqrt(mbuf1[slot, 1])
        from_row = pl.ds(pl.multiple_of(main + i * unit, unit), unit)
        for n in range(own_samples):
            noise = nz1[own_samples * c + n, from_row, :].astype(jnp.float32)
            value = mean + std * noise + low_rank[n * unit : (n + 1) * unit] * scale
            to = pl.ds(pl.multiple_of(samples * main + n * mid + i * unit, unit), unit)
            up[to, :] = value.astype(up.dtype)
        start_later(i + SLOTS)
        return carry

    pl.semaphore_wait(barrier, len(peers))

    lanes = pl.ds(pl.multiple_of(c * half, half), half)

    def low_copy():
        return remote(low_ref, lowbuf, sem_low, (), partner)

    def noise1_copy(i):
        src = pl.ds(pl.multiple_of((1 - c) * (main + mid) + i * unit, unit), unit)
        to = pl.ds(pl.multiple_of(i * unit, unit), unit)
        own = pl.ds(own_samples * c, own_samples)
        return remote(noise1_ref.at[:, src, :], nz1.at[own, to, :], sem_n1, (i,), partner)

    def noise1_arrival(i):
        src = pl.ds(pl.multiple_of((1 - c) * (main + mid) + i * unit, unit), unit)
        to = pl.ds(pl.multiple_of(i * unit, unit), unit)
        other = pl.ds(own_samples * (1 - c), own_samples)
        return remote(noise1_ref.at[:, src, :], nz1.at[other, to, :], sem_n1, (i,), partner)

    def noise2_copy(j):
        src = pl.ds(feature_row(1 - c, j), rows2)
        to = pl.ds(pl.multiple_of(j * rows2, rows2), rows2)
        own = pl.ds(own_samples * c, own_samples)
        return remote(noise2_ref.at[:, src, :], nz2.at[own, to, :], sem_n2, (j,), partner)

    def noise2_arrival(j):
        src = pl.ds(feature_row(1 - c, j), rows2)
        to = pl.ds(pl.multiple_of(j * rows2, rows2), rows2)
        other = pl.ds(own_samples * (1 - c), own_samples)
        return remote(noise2_ref.at[:, src, :], nz2.at[other, to, :], sem_n2, (j,), partner)

    def token_copy(shard, sems, index, device):
        ref = tok.at[shard, :, lanes]
        return remote(ref, ref, sems, index, device)

    own_rows = pl.ds(pl.multiple_of(x * (block // 2), block // 2), block // 2)
    other_rows = pl.ds(pl.multiple_of((1 - x) * (block // 2), block // 2), block // 2)

    def part_copy(shard, rows, sems, index, device):
        ref = tok.at[shard, rows, lanes]
        return remote(ref, ref, sems, index, device)

    def z_copy(k):
        if k == 1:
            return token_copy(s, sem_z, (k,), zn(k))
        return part_copy(s, own_rows, sem_z, (k,), zn(k))

    def z_arrival(k):
        if k == 1:
            return token_copy(s ^ 2, sem_z, (k,), zn(k))
        return part_copy(s ^ (2 * k), own_rows, sem_z, (k,), zn(k))

    def forward_copy():
        return part_copy(s ^ 4, own_rows, sem_z, (3,), zn(1))

    def y_copy(k):
        if k < 2:
            return token_copy(s ^ (2 * k), sem_y, (k,), yn)
        return part_copy(s ^ (2 * k), own_rows, sem_y, (k,), yn)

    def y_arrival(k):
        if k < 2:
            return token_copy(s ^ (2 * k) ^ 1, sem_y, (k,), yn)
        return part_copy(s ^ (2 * k) ^ 1, own_rows, sem_y, (k,), yn)

    def x_copy(k, side):
        return part_copy(s ^ (2 * k) ^ side, own_rows, sem_x, (k, side), xn)

    def x_arrival(k, side):
        return part_copy(s ^ (2 * k) ^ side, other_rows, sem_x, (k, side), xn)

    def d_copy(k, side):
        return token_copy(s ^ (2 * k) ^ side, sem_d, (k, side), partner)

    def d_arrival(k, side):
        other = pl.ds(pl.multiple_of((1 - c) * half, half), half)
        ref = tok.at[s ^ (2 * k) ^ side, :, other]
        return remote(ref, ref, sem_d, (k, side), partner)

    low_copy().start()
    y_copy(0).start()

    z_copy(2).start()
    z_copy(1).start()
    for i in range(n_main):
        noise1_copy(i).start()

    lax.fori_loop(0, n_mid, mid_step, 0)
    low_copy().wait_recv()
    others = spread_of(lowbuf[...])
    for i in range(own_samples):
        first = c == 0
        spread4[pl.ds(i * unit, unit), :] = jnp.where(first, mine[i], others[i])
        spread4[pl.ds((own_samples + i) * unit, unit), :] = jnp.where(first, others[i], mine[i])

    def main_step(i, carry):
        q = i + n_mid
        slot = q % SLOTS
        wait(copies1(q))
        noise1_arrival(i).wait_recv()
        stacked = dbuf1[slot].reshape(columns * unit, width)
        low_rank = jnp.dot(spread4[...], stacked, preferred_element_type=jnp.float32)
        mean = mbuf1[slot, 0]
        std = jnp.sqrt(mbuf1[slot, 1])
        from_row = pl.ds(pl.multiple_of(i * unit, unit), unit)
        for n in range(samples):
            noise = nz1[n, from_row, :].astype(jnp.float32)
            value = mean + std * noise + low_rank[n * unit : (n + 1) * unit] * scale
            up[pl.ds(pl.multiple_of(n * main + i * unit, unit), unit), :] = value.astype(up.dtype)
        start_later(q + SLOTS)
        noise2_copy(i).start()
        return carry

    def down_step(j, carry):
        slot = j % SLOTS
        wait(copies2(j))
        noise2_arrival(j).wait_recv()
        per_core = samples * main + own_samples * mid
        for u in range(rows2 // unit):
            inner = pl.ds(u * unit, unit)
            at = pl.ds(pl.multiple_of(j * rows2 + u * unit, unit), unit)
            stacked = dbuf2[slot, :, inner, :].reshape(columns * unit, hidden)
            low_rank = jnp.dot(spread4[...], stacked, preferred_element_type=jnp.float32)
            mean = mbuf2[slot, 0, inner, :]
            std = jnp.sqrt(mbuf2[slot, 1, inner, :])
            for n in range(samples):
                noise = nz2[n, at, :].astype(jnp.float32)
                value = mean + std * noise + low_rank[n * unit : (n + 1) * unit] * scale
                value = value.astype(down.dtype)
                holder, local = n // own_samples, n % own_samples
                down[at, pl.ds(n * main, main)] = value[:, :main]
                down[at, pl.ds(per_core + n * main, main)] = value[:, main + mid :]
                down[at, pl.ds(holder * per_core + samples * main + local * mid, mid)] = value[:, main : main + mid]
        start_later(n1 + j + SLOTS)
        return carry

    def hidden_copy(k):
        ref = hid.at[k, c]
        return remote(ref, ref, sem_h, (k,), partner)

    def hidden_arrival(k):
        ref = hid.at[k, 1 - c]
        return remote(ref, ref, sem_h, (k,), partner)

    across = (((1,), (1,)), ((), ()))

    def pre(k):
        zz = z ^ k
        if k:
            d_arrival(k, 0).wait_recv()
        d_arrival(k, 1).wait_recv()
        held = tok[pl.ds(2 * zz, 2), :, :].reshape(2 * block, width)

        size = hid.shape[2] // PRE_PARTS

        def rows_step(n, carry):
            at = pl.ds(pl.multiple_of(n * size, size), size)
            preact = lax.dot_general(up[at, :], held, across, preferred_element_type=jnp.float32)
            value = 0.5 * preact * (1.0 + lax.erf(preact * math.sqrt(0.5)))
            hid[k, c, at, :] = value.astype(hid.dtype)
            return carry

        lax.fori_loop(0, PRE_PARTS, rows_step, 0)
        hidden_copy(k).start()

    onward = jnp.where(c == 0, 1 - y, 0)

    def s1_copy(k, i):
        return remote(s1send.at[k, i], s1recv.at[k, i], sem_s1, (k, i), first_peer)

    def s2_copy(k):
        return remote(s2send.at[k], s2recv.at[k], sem_s2, (k,), second_peer)

    def s3_copy(k):
        return remote(s3send.at[k], s3recv.at[k], sem_s3, (k,), zn(k))

    def post(k):
        hidden_arrival(k).wait_recv()
        held = hid[k].reshape(down.shape[1], 2 * block)
        size = piece // POST_PARTS

        def rows_step(n, carry):
            kept, inner = n // POST_PARTS, n % POST_PARTS
            at = pl.ds(pl.multiple_of(n * size, size), size)
            to = pl.ds(pl.multiple_of(inner * size, size), size)
            total = jnp.dot(down[at, :], held, preferred_element_type=jnp.float32)
            for side in range(2):
                part[k, kept, side, to, :] = total[:, side * block : (side + 1) * block]
            return carry

        lax.fori_loop(0, 2 * POST_PARTS, rows_step, 0)
        for i in (onward, 1 - onward):
            value = part[k, jnp.where(c == 0, 0, i), jnp.where(c == 0, i, 1 - y)]
            s1send[k, i] = value.astype(s1send.dtype)
            s1_copy(k, i).start()

    def summed(k, i):
        s1_copy(k, i).wait_recv()
        value = part[k, jnp.where(c == 0, 1, i), jnp.where(c == 0, i, y)]
        return value + s1recv[k, i].astype(jnp.float32)

    def stage2(k):
        s2send[k] = summed(k, onward).astype(s2send.dtype)
        s2_copy(k).start()
        s2keep[k] = summed(k, 1 - onward)

    def stage3(k):
        s2_copy(k).wait_recv()
        value = s2keep[k] + s2recv[k].astype(jnp.float32)
        if k == 0:
            fin[...] = value
        else:
            s3send[k] = value.astype(s3send.dtype)
            s3_copy(k).start()

    def far_z(k):
        z_arrival(k).wait_recv()
        if k == 2:
            forward_copy().start()
        y_copy(k).start()
        x_copy(k, 0).start()

    def far_y(k):
        y_arrival(k).wait_recv()
        x_copy(k, 1).start()

    def far_x(k, side):
        x_arrival(k, side).wait_recv()
        d_copy(k, side).start()

    def near_z():
        z_arrival(1).wait_recv()
        d_copy(1, 0).start()

    def near_y(k):
        y_arrival(k).wait_recv()
        d_copy(k, 1).start()

    def sample_down(first, last):
        lax.fori_loop(first * n2 // 10, last * n2 // 10, down_step, 0)

    lax.fori_loop(0, 3 * n_main // 4, main_step, 0)
    far_z(2)
    lax.fori_loop(3 * n_main // 4, n_main, main_step, 0)
    for j in range(n_main, n2):
        noise2_copy(j).start()
    near_y(0)
    near_z()
    sample_down(0, 3)
    far_z(3)
    y_copy(1).start()
    far_x(2, 0)
    far_y(2)
    sample_down(3, 6)
    pre(0)
    sample_down(6, 10)
    far_x(3, 0)
    far_y(3)
    far_x(2, 1)
    post(0)
    near_y(1)
    pre(2)
    far_x(3, 1)
    pre(1)
    post(2)
    stage2(0)
    pre(3)
    post(1)
    post(3)
    stage2(2)
    stage3(0)
    stage2(1)
    stage3(2)
    stage2(3)
    stage3(1)
    stage3(3)
    result = fin[...]
    for k in range(1, steps):
        s3_copy(k).wait_recv()
        result = result + s3recv[k].astype(jnp.float32)
    result = result / total_samples
    out_ref[...] = result.astype(out_ref.dtype)

    low_copy().wait_send()
    for i in range(n_main):
        noise1_copy(i).wait_send()
    for j in range(n2):
        noise2_copy(j).wait_send()
    z_copy(1).wait_send()

    z_copy(2).wait_send()
    forward_copy().wait_send()
    for k in range(steps):
        y_copy(k).wait_send()
        d_copy(k, 1).wait_send()
        hidden_copy(k).wait_send()
        s1_copy(k, 0).wait_send()
        s1_copy(k, 1).wait_send()
        s2_copy(k).wait_send()
        if k:
            d_copy(k, 0).wait_send()
            s3_copy(k).wait_send()
        if k > 1:
            x_copy(k, 0).wait_send()
            x_copy(k, 1).wait_send()


def fused(
    tokens,
    fc1_mean,
    fc1_variance,
    fc1_deviation,
    fc2_mean,
    fc2_variance,
    fc2_deviation,
    noise_fc1,
    noise_fc2,
    noise_low,
):
    columns, hidden, width = fc1_deviation.shape
    own = noise_fc1.shape[0]
    samples = 2 * own
    groups = lax.axis_size("grp")
    shards = lax.axis_size("shard")
    steps = shards // 2
    block = tokens.shape[0]
    piece = width // groups
    tiles = hidden // 128
    main = tiles // 2 * 128
    mid = hidden - 2 * main
    unit = UNIT
    rows2 = 2 * unit
    n_main = main // unit
    n2 = 2 * piece // rows2
    per_core = samples * main + own * mid
    cfg = (unit, main, mid, rows2, 1.0 / math.sqrt(2.0 * (columns - 1)), own * groups)
    hbm = pl.BlockSpec(memory_space=pltpu.HBM)
    vmem = pl.BlockSpec(memory_space=pltpu.VMEM)
    bf16, f32 = jnp.bfloat16, jnp.float32
    dma = pltpu.SemaphoreType.DMA
    return pl.pallas_call(
        functools.partial(fused_kernel, cfg),
        out_shape=jax.ShapeDtypeStruct((piece, block), bf16),
        in_specs=[vmem] + [hbm] * 9,
        out_specs=vmem,
        scratch_shapes=[
            pltpu.VMEM(noise_low.shape, f32),
            pltpu.VMEM((samples * unit, columns * unit), bf16),
            pltpu.VMEM((own * unit, columns * unit), bf16),
            pltpu.VMEM((shards, block, width), bf16),
            pltpu.VMEM((SLOTS, columns, unit, width), bf16),
            pltpu.VMEM((SLOTS, 2, unit, width), f32),
            pltpu.VMEM((samples, main + mid, width), bf16),
            pltpu.VMEM((per_core, width), bf16),
            pltpu.VMEM((SLOTS, columns, rows2, hidden), bf16),
            pltpu.VMEM((SLOTS, 2, rows2, hidden), f32),
            pltpu.VMEM((samples, 2 * piece, hidden), bf16),
            pltpu.VMEM((2 * piece, 2 * per_core), bf16),
            pltpu.VMEM((steps, 2, per_core, 2 * block), bf16),
            pltpu.VMEM((steps, 2, 2, piece, block), f32),
            pltpu.VMEM((steps, 2, piece, block), bf16),
            pltpu.VMEM((steps, 2, piece, block), bf16),
            pltpu.VMEM((steps, piece, block), bf16),
            pltpu.VMEM((steps, piece, block), f32),
            pltpu.VMEM((steps, piece, block), bf16),
            pltpu.VMEM((steps, piece, block), bf16),
            pltpu.VMEM((steps, piece, block), bf16),
            pltpu.VMEM((piece, block), f32),
            dma((SLOTS, 4)),
            dma((SLOTS, 4)),
            dma,
            dma((2,)),
            dma((2, n_main)),
            dma((2, n2)),
            dma((2, steps)),
            dma((2, steps)),
            dma((2, steps, 2)),
            dma((2, steps, 2)),
            dma((2, steps)),
            dma((2, steps, 2)),
            dma((2, steps)),
            dma((2, steps)),
        ],
        compiler_params=pltpu.CompilerParams(
            collective_id=0, has_side_effects=True, vmem_limit_bytes=67043328
        ),
        name="swag",
    )(
        noise_low,
        tokens,
        fc1_mean,
        fc1_variance,
        fc1_deviation,
        fc2_mean,
        fc2_variance,
        fc2_deviation,
        noise_fc1,
        noise_fc2,
    ).T


def fits_fused(groups, shards, tokens, deviation):
    width, hidden = tokens.shape[1], deviation.shape[1]
    return (
        groups == 4
        and shards == 8
        and hidden % 128 == 0
        and hidden // 128 % 2 == 1
        and width % 256 == 0
        and width // groups % (2 * UNIT) == 0
        and tokens.shape[0] % 128 == 0
    )


def body(
    tokens,
    fc1_mean,
    fc1_variance,
    fc1_deviation,
    fc2_mean,
    fc2_variance,
    fc2_deviation,
    noise_fc1,
    noise_fc2,
    noise_low,
):
    groups = lax.axis_size("grp")
    shard_count = lax.axis_size("shard")
    if fits_fused(groups, shard_count, tokens, fc1_deviation):
        return fused(
            tokens,
            fc1_mean,
            fc1_variance,
            fc1_deviation,
            fc2_mean,
            fc2_variance,
            fc2_deviation,
            noise_fc1,
            noise_fc2,
            noise_low,
        )
    low_half = noise_low.astype(jnp.bfloat16)
    samples = noise_fc1.shape[0] * groups
    hid_ways = min(8, shard_count)
    low_bits = (shard_count // hid_ways).bit_length() - 1
    tok_bits = hid_ways.bit_length() - 1
    grp_bits = groups.bit_length() - 1
    position = lax.axis_index("shard")
    group = lax.axis_index("grp")
    core = group % 2
    rows, width = tokens.shape
    half = width // 2

    mine = lax.dynamic_slice_in_dim(tokens, core * half, half, 1)
    gathered = [mine] + [from_partner(mine, "shard", m << low_bits) for m in range(1, hid_ways)]

    order = jnp.bitwise_xor(jnp.arange(groups, dtype=jnp.int32), group.astype(jnp.int32))
    whole = jnp.zeros((1,), jnp.int32)
    up = sample_weights(whole, 1, fc1_mean, fc1_variance, fc1_deviation, noise_fc1, low_half, "sample_up")
    down = sample_weights(order, groups, fc2_mean, fc2_variance, fc2_deviation, noise_fc2, low_half, "sample_down")
    for bit in range(low_bits):
        upper = position >> bit & 1 == 1
        partner = from_partner(up, "shard", 1 << bit)
        up = jnp.where(upper, jnp.concatenate([partner, up], 1), jnp.concatenate([up, partner], 1))
        partner = from_partner(down, "shard", 1 << bit)
        down = jnp.where(upper, jnp.concatenate([partner, down], 2), jnp.concatenate([down, partner], 2))

    gathered, up, down = lax.optimization_barrier((gathered, up, down))
    own = jnp.concatenate(gathered, 0)
    other = from_partner(own, "grp", 1)
    piece = width // groups
    kept_and_sent = mlp(core.astype(jnp.int32).reshape(1), own, other, up, down, groups, rows)
    grp_steps = [("grp", 1 << b, grp_bits - 1 - b) for b in range(1, grp_bits)]
    shard_steps = [("shard", 1 << (low_bits + b), grp_bits + tok_bits - 2 - b) for b in range(tok_bits)]
    first, second, rest = grp_steps, shard_steps[:1], shard_steps[:0:-1]
    done = []
    for stream, steps in enumerate((first + second + rest, second + first + rest)):
        swapped = from_partner(kept_and_sent[2 + stream], "grp", 1)
        part = kept_and_sent[stream].astype(jnp.float32) + swapped.astype(jnp.float32)
        part = part.reshape((2,) * (grp_bits - 1 + tok_bits) + (rows // 2, piece))
        for axis, mask, dim in steps:
            part = fold(part.astype(jnp.bfloat16), axis, mask, dim)
        done.append(part.reshape(rows // 2, piece))
    return (jnp.concatenate(done, 0) / samples).astype(jnp.bfloat16)


def solution(mesh):
    placed = (
        P("shard", None),
        P("shard", None),
        P("shard", None),
        P(None, "shard", None),
        P(None, "shard"),
        P(None, "shard"),
        P(None, None, "shard"),
        P("grp", "shard", None),
        P("grp", None, "shard"),
        P("grp", None),
    )
    return jax.shard_map(
        body, mesh=mesh, in_specs=placed, out_specs=P("shard", "grp"), check_vma=False
    )
```
